32 devices in a mesh: section: 4 (over x, core), tensor: 4 (over z), dp: 2 (over y).
Axes of the slice: x: 2, y: 2, z: 4, core: 2. Of those that a mesh axis runs over, the one named last changes fastest.
Arguments:
- layer_in: bfloat16 [2, 2, 4, 2, 128, 2560], P(None, None, 'section', 'dp', 'tensor'), may hold values from -6 to 6
- carry_in: bfloat16 [2, 4, 2, 128, 2560], P(None, 'section', 'dp', 'tensor'), may hold values from -6 to 6
- top_grad: bfloat16 [1, 2, 128, 2560], P(None, 'dp', 'tensor'), may hold values from -6 to 6
- w_qkv: bfloat16 [2, 4, 2560, 2560], P(None, 'section', None, 'tensor'), may hold values from -1 to 1
- w_out: bfloat16 [2, 4, 2048, 2560], P(None, 'section', 'tensor'), may hold values from -0.125 to 0.125
- gain: float32 [2, 4, 2560], P(None, 'section'), may hold values from 0.5 to 1.5
Outputs:
- unit_grads: bfloat16 [2, 2, 4, 2, 128, 2560], P(None, None, 'section', 'dp', 'tensor')
- grad_qkv: bfloat16 [2, 4, 2560, 2560], P(None, 'section', 'dp', 'tensor')
- grad_out: bfloat16 [2, 4, 2048, 2560], P(None, 'section', ('tensor', 'dp'))
- grad_gain: float32 [2, 4, 2560], P(None, 'section')
The draws below stay inside these ranges and needn't reach their ends.
All inputs are finite; a program needn't handle non-finite values.
Results may differ from the reference program's by a relative error of at most 0.022.
The reference program's roundings to bfloat16 on the way count: a program that leaves them out, or rounds other values in their place, can miss the bound.
Values may be sent and summed in bfloat16 or wider, within the bound.
No kernel may reach another device: no remote copies, remote signals or barrier semaphores. Data moves between devices by JAX's collectives and lax.ppermute only.
A program may use at most 128 MiB of HBM per device.

```python
import math
import jax
import jax.numpy as jnp
from jax import lax

D = 2560
KV = 4
HD = 64
SEQ = 128
TICKS = 2
GROUP = 8
HQ = 2048
QKV = 2560
SECTIONS = 4
REPLICAS = 2
N_TENSOR = 4


def draw_w_qkv(key, part):
    draw_shape = (2, SECTIONS, D, KV, GROUP + 2, HD)
    entries = jax.random.normal(key, draw_shape, jnp.float32) / jnp.sqrt(jnp.float32(D))
    return jnp.clip(entries, -1.0, 1.0).reshape(2, SECTIONS, D, KV * (GROUP + 2) * HD).astype(jnp.bfloat16)


def level_of(stream_key, shape, pieces, smallest, largest):
    def one(axis_at, parts):
        steps = jax.random.uniform(jax.random.fold_in(jax.random.fold_in(stream_key, 6), axis_at), (parts,), jnp.float32, smallest / len(pieces), largest / len(pieces))
        return jnp.repeat(jnp.exp(steps), shape[axis_at] // parts).reshape((-1,) + (1,) * (len(shape) - axis_at - 1))

    factor_of = one(*pieces[0])
    for cut in pieces[1:]:
        factor_of = factor_of * one(*cut)
    return factor_of


def gaussian(own_key, extent, spread, most, cuts=(), kind=jnp.bfloat16):
    values = spread * jax.random.normal(own_key, extent, jnp.float32)
    if cuts:
        values = values * level_of(own_key, extent, cuts, -0.22, 0.18)
    return jnp.clip(values, -most, most).astype(kind)


def setup_inputs(seed: int = 0) -> dict:
    arg_keys = jax.random.split(jax.random.key(seed), 7)
    return {
        "layer_in": gaussian(arg_keys[0], (TICKS, 2, SECTIONS, REPLICAS, SEQ, D), 1.0, 6.0, ((2, 4), (3, 2), (4, 4))),
        "carry_in": gaussian(arg_keys[1], (2, SECTIONS, REPLICAS, SEQ, D), 1.0, 6.0, ((1, 4), (2, 2), (3, 4))),
        "top_grad": gaussian(arg_keys[2], (TICKS - 1, REPLICAS, SEQ, D), 1.0, 6.0, ((1, 2), (2, 4))),
        "w_qkv": draw_w_qkv(jax.random.fold_in(arg_keys[6], 71), 0),
        "w_out": gaussian(arg_keys[4], (2, SECTIONS, HQ, D), HQ ** -0.5, 0.125, ((1, 4), (2, 4))),
        "gain": jnp.clip(1.0 + 0.1 * jax.random.normal(arg_keys[5], (2, SECTIONS, D), jnp.float32), 0.5, 1.5),
    }


epsilon = 1e-06
rope_base = 1000000.0

def rope_tables(length, head_width):
    half_width = head_width // 2
    exponent = jnp.arange(half_width, dtype=jnp.float32) * (2.0 / head_width)
    frequency = rope_base ** (-exponent)
    angle = jnp.arange(length, dtype=jnp.float32)[:, None] * frequency[None, :]
    return (jnp.cos(angle), jnp.sin(angle))

def rotate(values, cosine_table, sine_table, direction):
    half_width = values.shape[-1] // 2
    table_shape = (values.shape[0],) + (1,) * (values.ndim - 2) + (half_width,)
    cosine = cosine_table.reshape(table_shape)
    sine_part = direction * sine_table.reshape(table_shape)
    lower_half = values[..., :half_width]
    upper_half = values[..., half_width:]
    return jnp.concatenate([lower_half * cosine - upper_half * sine_part, upper_half * cosine + lower_half * sine_part], axis=-1)

def layer_backward(layer_rows, grad_output, weight_qkv, weight_out, gain_row):
    length = layer_rows.shape[0]
    cosine_table, sine_table = rope_tables(length, HD)
    inputs_float = layer_rows.astype(jnp.float32)
    inverse = lax.rsqrt(lax.optimization_barrier(jnp.mean(inputs_float * inputs_float, axis=-1, keepdims=True)) + epsilon)
    unit_rows = inputs_float * inverse
    normed = (unit_rows * gain_row).astype(jnp.bfloat16)
    projected = jnp.dot(normed, weight_qkv, preferred_element_type=jnp.float32).reshape(length, KV, GROUP + 2, HD)
    query_rot = rotate(projected[:, :, :GROUP], cosine_table, sine_table, 1.0).astype(jnp.bfloat16)
    key_rot = rotate(projected[:, :, GROUP], cosine_table, sine_table, 1.0).astype(jnp.bfloat16)
    value_rows = projected[:, :, GROUP + 1].astype(jnp.bfloat16)
    query_float = query_rot.astype(jnp.float32)
    key_float = key_rot.astype(jnp.float32)
    value_float = value_rows.astype(jnp.float32)
    score_scale = 1.0 / math.sqrt(HD)
    scores = jnp.einsum('tkgd,ukd->kgtu', query_float, key_float) * score_scale
    causal_mask = jnp.arange(length)[:, None] >= jnp.arange(length)[None, :]
    scores = jnp.where(causal_mask, scores, -1e+30)
    exponentials = jnp.exp(scores - lax.optimization_barrier(jnp.max(scores, axis=-1, keepdims=True)))
    softmax_rows = exponentials / lax.optimization_barrier(jnp.sum(exponentials, axis=-1, keepdims=True))
    softmax_low = softmax_rows.astype(jnp.bfloat16)
    softmax_float = softmax_low.astype(jnp.float32)
    attended = jnp.einsum('kgtu,ukd->tkgd', softmax_float, value_float).astype(jnp.bfloat16).reshape(length, HQ)
    grad_attended = jnp.dot(grad_output, weight_out.T, preferred_element_type=jnp.float32).astype(jnp.bfloat16)
    grad_heads = grad_attended.reshape(length, KV, GROUP, HD).astype(jnp.float32)
    grad_softmax = jnp.einsum('tkgd,ukd->kgtu', grad_heads, value_float)
    row_total = lax.optimization_barrier(jnp.sum(softmax_rows * grad_softmax, axis=-1, keepdims=True))
    grad_scores = (softmax_rows * (grad_softmax - row_total) * score_scale).astype(jnp.bfloat16)
    grad_score_float = grad_scores.astype(jnp.float32)
    grad_value = jnp.einsum('kgtu,tkgd->ukd', softmax_float, grad_heads)
    grad_query = rotate(jnp.einsum('kgtu,ukd->tkgd', grad_score_float, key_float), cosine_table, sine_table, -1.0)
    grad_key = rotate(jnp.einsum('kgtu,tkgd->ukd', grad_score_float, query_float), cosine_table, sine_table, -1.0)
    grad_projected = jnp.concatenate([grad_query, grad_key[:, :, None], grad_value[:, :, None]], axis=2)
    grad_projected = grad_projected.reshape(length, QKV).astype(jnp.bfloat16)
    block_width = QKV // N_TENSOR
    grad_normed = jnp.zeros((length, D), jnp.float32)
    for column_block in range(N_TENSOR):
        lower = column_block * block_width
        block_term = jnp.dot(grad_projected[:, lower:lower + block_width], weight_qkv[:, lower:lower + block_width].T, preferred_element_type=jnp.float32)
        grad_normed = grad_normed + block_term.astype(jnp.bfloat16).astype(jnp.float32)
    grad_unit = grad_normed * gain_row
    grad_rows = inverse * (grad_unit - unit_rows * lax.optimization_barrier(jnp.mean(grad_unit * unit_rows, axis=-1, keepdims=True)))
    grad_input = (grad_output.astype(jnp.float32) + grad_rows).astype(jnp.bfloat16)
    grad_scale = lax.optimization_barrier(jnp.sum(grad_normed * unit_rows, axis=0))
    grad_wqkv = jnp.dot(normed.T, grad_projected, preferred_element_type=jnp.float32)
    grad_wout = jnp.dot(attended.T, grad_output, preferred_element_type=jnp.float32)
    return (grad_input, grad_wqkv, grad_wout, grad_scale)

def reference(layer_in, carry_in, top_grad, w_qkv, w_out, gain):
    ticks = layer_in.shape[0]
    sections = layer_in.shape[2]
    per_replica = (jnp.moveaxis(layer_in, 3, 0), jnp.moveaxis(carry_in, 2, 0), jnp.moveaxis(top_grad, 1, 0))

    def one_replica(totals, slices):
        layer_rows, carried, fresh_grads = slices
        sum_qkv = jnp.zeros(w_qkv.shape, jnp.float32)
        sum_out = jnp.zeros(w_out.shape, jnp.float32)
        gain_total = totals[2]
        produced = {}
        per_tick = []
        for position in range(ticks):
            current = {}
            for member in (1, 0):
                for section_index in range(sections):
                    if position == 0:
                        incoming = carried[member, section_index]
                    elif member == 1 and section_index == 0:
                        incoming = fresh_grads[position - 1]
                    elif member == 1:
                        incoming = produced[1, section_index - 1]
                    elif section_index == sections - 1:
                        incoming = produced[1, section_index]
                    else:
                        incoming = produced[0, section_index + 1]
                    outcome = layer_backward(layer_rows[position, member, section_index], incoming, w_qkv[member, section_index], w_out[member, section_index], gain[member, section_index])
                    current[member, section_index] = outcome[0]
                    sum_qkv = sum_qkv.at[member, section_index].add(outcome[1])
                    sum_out = sum_out.at[member, section_index].add(outcome[2])
                    gain_total = gain_total.at[member, section_index].add(outcome[3])
            produced = current
            per_tick.append(jnp.stack([jnp.stack([current[member, index] for index in range(sections)]) for member in (0, 1)]))
        new_qkv = totals[0] + sum_qkv.astype(jnp.bfloat16).astype(jnp.float32)
        new_out = totals[1] + sum_out.astype(jnp.bfloat16).astype(jnp.float32)
        return ((new_qkv, new_out, gain_total), jnp.stack(per_tick))
    start_totals = (jnp.zeros(w_qkv.shape, jnp.float32), jnp.zeros(w_out.shape, jnp.float32), jnp.zeros(gain.shape, jnp.float32))
    totals, grads_all = lax.scan(one_replica, start_totals, per_replica)
    unit_grads = jnp.moveaxis(grads_all, 0, 3)
    return (unit_grads, totals[0].astype(jnp.bfloat16), totals[1].astype(jnp.bfloat16), totals[2])
```

```python
import math

import jax
import jax.numpy as jnp
from jax import lax
from jax.sharding import PartitionSpec as P

HD = 64
GROUP = 8

epsilon = 1e-06
rope_base = 1000000.0


ROWS = (((0,), (0,)), ((), ()))
COLS = (((1,), (1,)), ((), ()))


def rope_tables(length, head_width):
    half_width = head_width // 2
    exponent = jnp.arange(half_width, dtype=jnp.float32) * (2.0 / head_width)
    frequency = rope_base ** (-exponent)
    angle = jnp.arange(length, dtype=jnp.float32)[:, None] * frequency[None, :]
    return (jnp.cos(angle), jnp.sin(angle))


def rotate(values, cosine_table, sine_table, direction):
    half_width = values.shape[-1] // 2
    table_shape = (values.shape[0],) + (1,) * (values.ndim - 2) + (half_width,)
    cosine = cosine_table.reshape(table_shape)
    sine_part = direction * sine_table.reshape(table_shape)
    lower_half = values[..., :half_width]
    upper_half = values[..., half_width:]
    return jnp.concatenate(
        [
            lower_half * cosine - upper_half * sine_part,
            upper_half * cosine + lower_half * sine_part,
        ],
        axis=-1,
    )


def shift(value, axis, steps):
    count = lax.axis_size(axis)
    return lax.ppermute(value, axis, [(i, (i + steps) % count) for i in range(count)])


def sum_over(value, axis):
    count = lax.axis_size(axis)
    if count & (count - 1):
        return lax.psum(value, axis)
    step = 1
    while step < count:
        value = value + lax.ppermute(value, axis, [(i, i ^ step) for i in range(count)])
        step *= 2
    return value


def gather_rotated(value):
    count = lax.axis_size("tensor")
    return [value] + [shift(value, "tensor", k) for k in range(1, count)]


def local(layer_in, carry_in, top_grad, w_qkv, w_out, gain):
    ticks = layer_in.shape[0]
    own_rows = layer_in.shape[4]
    width = layer_in.shape[5]
    nt = lax.axis_size("tensor")
    ns = lax.axis_size("section")
    nd = lax.axis_size("dp")
    length = own_rows * nt
    section = lax.axis_index("section")
    place = lax.axis_index("tensor")
    replica = lax.axis_index("dp")
    at_first = section == 0
    at_last = section == ns - 1
    score_scale = 1.0 / math.sqrt(HD)
    x_rows = layer_in[:, :, 0, 0]
    carried = carry_in[:, 0, 0]
    fresh_rows = top_grad[:, 0]
    weight_qkv = w_qkv[:, 0]
    weight_out = w_out[:, 0]
    gain_rows = gain[:, 0]
    kv_local = weight_qkv.shape[2] // ((GROUP + 2) * HD)
    members = (1, 0)

    def rotated(table):
        blocks = table.reshape((nt, own_rows) + table.shape[1:])[::-1]
        twice = jnp.concatenate([blocks, blocks], axis=0)
        picked = lax.dynamic_slice_in_dim(twice, nt - 1 - place, nt, axis=0)
        return picked.reshape(table.shape)

    cosine_table, sine_table = (rotated(t) for t in rope_tables(length, HD))
    positions = rotated(jnp.arange(length)[:, None])[:, 0]
    causal_mask = positions[:, None] >= positions[None, :]

    def st(s, t):
        return s * nt + t % nt

    def hop(value, moves):
        outs = []
        for k in range(nt):
            pairs = [(st(a, t), st(b, t + k)) for a, b in moves for t in range(nt)]
            outs.append(lax.ppermute(value, ("section", "tensor"), pairs))
        return outs

    def stay(value, a):
        outs = [value]
        for k in range(1, nt):
            pairs = [(st(a, t), st(a, t + k)) for t in range(nt)]
            outs.append(lax.ppermute(value, ("section", "tensor"), pairs))
        return outs

    def join(parts):
        return jnp.concatenate(parts, axis=0)

    def normalize(rows):
        rows = rows.astype(jnp.float32)
        inverse = lax.rsqrt(jnp.mean(rows * rows, axis=-1, keepdims=True) + epsilon)
        return rows * inverse, inverse

    def slice_for(value, p, axis):
        extent = value.shape[axis] // nd
        return lax.dynamic_slice_in_dim(value, ((replica + p) % nd) * extent, extent, axis=axis)

    def to_peers(value, axis=None):
        outs = []
        for p in range(1, nd):
            part = value if axis is None else slice_for(value, p, axis)
            outs.append(shift(part, "dp", p))
        return outs

    def forward(x_full, member):
        unit_rows, _ = normalize(x_full)
        normed = (unit_rows * gain_rows[member]).astype(jnp.bfloat16)
        projected = jnp.dot(normed, weight_qkv[member], preferred_element_type=jnp.float32)
        projected = projected.reshape(length, kv_local, GROUP + 2, HD)
        query_rot = rotate(projected[:, :, :GROUP], cosine_table, sine_table, 1.0)
        query_rot = query_rot.astype(jnp.bfloat16)
        key_rot = rotate(projected[:, :, GROUP], cosine_table, sine_table, 1.0)
        key_rot = key_rot.astype(jnp.bfloat16)
        value_rows = projected[:, :, GROUP + 1].astype(jnp.bfloat16)
        scores = (
            jnp.einsum("tkgd,ukd->kgtu", query_rot, key_rot, preferred_element_type=jnp.float32)
            * score_scale
        )
        scores = jnp.where(causal_mask, scores, -1e30)
        exponentials = jnp.exp(scores - jnp.max(scores, axis=-1, keepdims=True))
        softmax_rows = exponentials / jnp.sum(exponentials, axis=-1, keepdims=True)
        softmax_low = softmax_rows.astype(jnp.bfloat16)
        attended = jnp.einsum(
            "kgtu,ukd->tkgd", softmax_low, value_rows, preferred_element_type=jnp.float32
        )
        attended = attended.astype(jnp.bfloat16).reshape(length, kv_local * GROUP * HD)
        return normed, attended, (query_rot, key_rot, value_rows, softmax_rows, softmax_low)

    def backward(saved, grad_full, member):
        query_rot, key_rot, value_rows, softmax_rows, softmax_low = saved
        grad_attended = lax.dot_general(
            grad_full, weight_out[member], COLS, preferred_element_type=jnp.float32
        ).astype(jnp.bfloat16)
        grad_heads = grad_attended.reshape(length, kv_local, GROUP, HD)
        grad_softmax = jnp.einsum(
            "tkgd,ukd->kgtu", grad_heads, value_rows, preferred_element_type=jnp.float32
        )
        row_total = jnp.sum(softmax_rows * grad_softmax, axis=-1, keepdims=True)
        grad_scores = (softmax_rows * (grad_softmax - row_total) * score_scale).astype(
            jnp.bfloat16
        )
        grad_value = jnp.einsum(
            "kgtu,tkgd->ukd", softmax_low, grad_heads, preferred_element_type=jnp.float32
        )
        grad_query = rotate(
            jnp.einsum(
                "kgtu,ukd->tkgd", grad_scores, key_rot, preferred_element_type=jnp.float32
            ),
            cosine_table,
            sine_table,
            -1.0,
        )
        grad_key = rotate(
            jnp.einsum(
                "kgtu,tkgd->ukd", grad_scores, query_rot, preferred_element_type=jnp.float32
            ),
            cosine_table,
            sine_table,
            -1.0,
        )
        grad_projected = jnp.concatenate(
            [grad_query, grad_key[:, :, None], grad_value[:, :, None]], axis=2
        )
        grad_projected = grad_projected.reshape(length, -1).astype(jnp.bfloat16)
        partial = lax.dot_general(
            grad_projected, weight_qkv[member], COLS, preferred_element_type=jnp.float32
        ).astype(jnp.bfloat16)
        return grad_projected, partial

    def scatter_rotated(partial):
        blocks = partial.reshape(nt, own_rows, width)
        total = blocks[0].astype(jnp.float32)
        for k in range(1, nt):
            total = total + shift(blocks[k], "tensor", -k).astype(jnp.float32)
        return total

    x_full = [[None, None] for _ in range(ticks)]
    grads_in = [None, None]
    for member in members:
        x_full[0][member] = join(gather_rotated(x_rows[0, member]))
        grads_in[member] = gather_rotated(carried[member])
    fresh_full = [join(stay(fresh_rows[t], 0)) for t in range(ticks - 1)]
    for t in range(1, ticks):
        for member in members:
            x_full[t][member] = join(gather_rotated(x_rows[t, member]))

    own_grads = [g[0] for g in grads_in]
    grads_full = [join(g) for g in grads_in]
    normed_all = ([], [])
    peer_normed = ([], [])
    attended_all = ([], [])
    peer_attended = ([], [])
    grads_all = ([], [])
    peer_grads = ([], [])
    projected_all = ([], [])
    peer_projected = ([], [])
    gain_totals = [0.0, 0.0]
    per_tick = []
    for t in range(ticks):
        outcome = [None, None]
        for member in members:
            normed, attended, saved = forward(x_full[t][member], member)
            normed_all[member].append(slice_for(normed, 0, 1))
            peer_normed[member].extend(to_peers(normed, 1))
            attended_all[member].append(slice_for(attended, 0, 1))
            peer_attended[member].extend(to_peers(attended, 1))
            grad_full = grads_full[member]
            grads_all[member].append(grad_full)
            peer_grads[member].extend(to_peers(grad_full))
            grad_projected, partial = backward(saved, grad_full, member)
            projected_all[member].append(grad_projected)
            peer_projected[member].extend(to_peers(grad_projected))
            unit_rows, _ = normalize(x_full[t][member])
            gain_totals[member] = gain_totals[member] + jnp.sum(
                partial.astype(jnp.float32) * unit_rows, axis=0
            )
            grad_normed = scatter_rotated(partial)
            unit_own, inverse = normalize(x_rows[t, member])
            grad_unit = grad_normed * gain_rows[member]
            grad_rows = inverse * (
                grad_unit - unit_own * jnp.mean(grad_unit * unit_own, axis=-1, keepdims=True)
            )
            outcome[member] = (own_grads[member].astype(jnp.float32) + grad_rows).astype(
                jnp.bfloat16
            )
        if t + 1 < ticks:
            from_below = hop(outcome[1], [(s, s + 1) for s in range(ns - 1)])
            from_above = hop(outcome[0], [(s, s - 1) for s in range(1, ns)])
            turned = stay(outcome[1], ns - 1)
            own_grads = [
                jnp.where(at_last, turned[0], from_above[0]),
                jnp.where(at_first, fresh_rows[t], from_below[0]),
            ]
            grads_full = [
                jnp.where(at_last, join(turned), join(from_above)),
                jnp.where(at_first, fresh_full[t], join(from_below)),
            ]
        per_tick.append(jnp.stack(outcome))

    grad_qkv = jnp.stack(
        [
            lax.dot_general(
                join(normed_all[m] + peer_normed[m]),
                join(projected_all[m] + peer_projected[m]),
                ROWS,
                preferred_element_type=jnp.float32,
            ).astype(jnp.bfloat16)
            for m in (0, 1)
        ]
    )
    grad_out = jnp.stack(
        [
            lax.dot_general(
                join(attended_all[m] + peer_attended[m]),
                join(grads_all[m] + peer_grads[m]),
                ROWS,
                preferred_element_type=jnp.float32,
            ).astype(jnp.bfloat16)
            for m in (0, 1)
        ]
    )
    gain_total = jnp.stack(gain_totals)
    for axis in ("tensor", "dp"):
        gain_total = sum_over(gain_total, axis)
    return (
        jnp.stack(per_tick)[:, :, None, None],
        grad_qkv[:, None],
        grad_out[:, None],
        gain_total[:, None],
    )


def solution(mesh):
    in_specs = (
        P(None, None, "section", "dp", "tensor", None),
        P(None, "section", "dp", "tensor", None),
        P(None, "dp", "tensor", None),
        P(None, "section", None, "tensor"),
        P(None, "section", "tensor", None),
        P(None, "section", None),
    )
    out_specs = (
        P(None, None, "section", "dp", "tensor", None),
        P(None, "section", "dp", "tensor"),
        P(None, "section", ("tensor", "dp"), None),
        P(None, "section", None),
    )
    return jax.shard_map(local, mesh=mesh, in_specs=in_specs, out_specs=out_specs, check_vma=False)
```

```python
import functools
import math

import jax
import jax.numpy as jnp
from jax import lax
from jax.experimental import pallas as pl
from jax.experimental.pallas import tpu as pltpu
from jax.sharding import PartitionSpec as P


HD = 64
GROUP = 8

epsilon = 1e-06
rope_base = 1000000.0


ROWS = (((0,), (0,)), ((), ()))
COLS = (((1,), (1,)), ((), ()))
VMEM_BYTES = 28 * 1024 * 1024


def swap_halves(values, lane):
    width = values.shape[-1]
    half = HD // 2
    ahead = pltpu.roll(values, width - half, 1)
    behind = pltpu.roll(values, half, 1)
    return jnp.where(lane % HD < half, ahead, behind)


def pair_up(values, lane):
    low = jnp.where(lane < HD, values, 0.0)
    high = pltpu.roll(low, HD, 1)
    return jnp.concatenate([low, high], axis=0).astype(jnp.bfloat16)


def forward_kernel(nt, kv_local, *refs):
    parts, rest = refs[:nt], refs[nt:]
    gain_ref, *weight_refs, cos_ref, sin_ref, bias_ref = rest[:6]
    normed_ref, attended_ref, rotated_ref, softmax_ref = rest[6:]
    cosine, sine, bias = cos_ref[...], sin_ref[...], bias_ref[...]
    scale = 1.0 / math.sqrt(HD)
    chunks = GROUP // 2
    for m in range(2):
        rows = jnp.concatenate([p[m].astype(jnp.float32) for p in parts], axis=0)
        inverse = lax.rsqrt(jnp.mean(rows * rows, axis=-1, keepdims=True) + epsilon)
        normed = (rows * inverse * gain_ref[m]).astype(jnp.bfloat16)
        normed_ref[m] = normed
        projected = jnp.dot(normed, weight_refs[m][...], preferred_element_type=jnp.float32)
        length = rows.shape[0]
        lane = lax.broadcasted_iota(jnp.int32, (length, 2 * HD), 1)
        for group in range(kv_local):
            base = group * (GROUP + 2) * HD
            at = base + GROUP * HD
            pair = projected[:, at : at + 2 * HD]
            turned = pair * cosine + swap_halves(pair, lane) * sine
            key_value = jnp.where(lane < HD, turned, pair)
            rotated_ref[m, :, at : at + 2 * HD] = key_value.astype(jnp.bfloat16)
            keys = pair_up(key_value, lane)
            values = pair_up(pltpu.roll(key_value, HD, 1), lane)
            for c in range(chunks):
                lo = base + c * 2 * HD
                heads = projected[:, lo : lo + 2 * HD]
                query = (heads * cosine + swap_halves(heads, lane) * sine).astype(jnp.bfloat16)
                rotated_ref[m, :, lo : lo + 2 * HD] = query
                scores = lax.dot_general(query, keys, COLS, preferred_element_type=jnp.float32)
                softmax = []
                for h in range(2):
                    one = scores[:, h * length : (h + 1) * length] * scale + bias
                    power = jnp.exp(one - jnp.max(one, axis=-1, keepdims=True))
                    softmax.append(power / jnp.sum(power, axis=-1, keepdims=True))
                softmax = jnp.concatenate(softmax, axis=1)
                so = (group * chunks + c) * 2 * length
                softmax_ref[m, :, so : so + 2 * length] = softmax
                attended = jnp.dot(
                    softmax.astype(jnp.bfloat16), values, preferred_element_type=jnp.float32
                )
                ao = (group * chunks + c) * 2 * HD
                attended_ref[m, :, ao : ao + 2 * HD] = attended.astype(jnp.bfloat16)


def backward_kernel(nt, kv_local, *refs):
    parts, rest = refs[:nt], refs[nt:]
    wout_refs, wqkv_refs = rest[0:2], rest[2:4]
    rotated_ref, softmax_ref, cos_ref, sin_ref, projected_ref = rest[4:9]
    partial_refs = rest[9:]
    own = parts[0].shape[1]
    length = own * nt
    lane = lax.broadcasted_iota(jnp.int32, (length, 2 * HD), 1)
    cosine, sine = cos_ref[...], sin_ref[...]
    scale = 1.0 / math.sqrt(HD)
    chunks = GROUP // 2

    def unturn(values):
        return values * cosine - swap_halves(values, lane) * sine

    for m in (1, 0):
        grad_full = jnp.concatenate([p[m] for p in parts], axis=0)
        grad_attended = lax.dot_general(
            grad_full, wout_refs[m][...], COLS, preferred_element_type=jnp.float32
        ).astype(jnp.bfloat16)
        for group in range(kv_local):
            base = group * (GROUP + 2) * HD
            at = base + GROUP * HD
            key_value = rotated_ref[m, :, at : at + 2 * HD].astype(jnp.float32)
            keys = pair_up(key_value, lane)
            values = pair_up(pltpu.roll(key_value, HD, 1), lane)
            key_sum = jnp.zeros((2 * length, 2 * HD), jnp.float32)
            value_sum = jnp.zeros((2 * length, 2 * HD), jnp.float32)
            for c in range(chunks):
                lo = base + c * 2 * HD
                ao = (group * chunks + c) * 2 * HD
                so = (group * chunks + c) * 2 * length
                grad_heads = grad_attended[:, ao : ao + 2 * HD]
                softmax = softmax_ref[m, :, so : so + 2 * length]
                grad_softmax = lax.dot_general(
                    grad_heads, values, COLS, preferred_element_type=jnp.float32
                )
                grad_scores = []
                for h in range(2):
                    here = slice(h * length, (h + 1) * length)
                    sm, gs = softmax[:, here], grad_softmax[:, here]
                    total = jnp.sum(sm * gs, axis=-1, keepdims=True)
                    grad_scores.append((sm * (gs - total) * scale).astype(jnp.bfloat16))
                grad_scores = jnp.concatenate(grad_scores, axis=1)
                grad_query = jnp.dot(grad_scores, keys, preferred_element_type=jnp.float32)
                projected_ref[m, :, lo : lo + 2 * HD] = unturn(grad_query).astype(jnp.bfloat16)
                query = rotated_ref[m, :, lo : lo + 2 * HD]
                key_sum = key_sum + lax.dot_general(
                    grad_scores, query, ROWS, preferred_element_type=jnp.float32
                )
                value_sum = value_sum + lax.dot_general(
                    softmax.astype(jnp.bfloat16),
                    grad_heads,
                    ROWS,
                    preferred_element_type=jnp.float32,
                )
            grad_key = unturn(key_sum[:length] + pltpu.roll(key_sum[length:], HD, 1))
            grad_value = pltpu.roll(value_sum[:length], HD, 1) + value_sum[length:]
            projected_ref[m, :, at : at + 2 * HD] = jnp.where(
                lane < HD, grad_key, grad_value
            ).astype(jnp.bfloat16)
        partial = lax.dot_general(
            projected_ref[m], wqkv_refs[m][...], COLS, preferred_element_type=jnp.float32
        ).astype(jnp.bfloat16)
        for k in range(nt):
            partial_refs[k][m] = partial[k * own : (k + 1) * own]


def gain_kernel(nt, *refs):
    for m in range(2):
        total = None
        for k in range(nt):
            rows = refs[k][m].astype(jnp.float32)
            inverse = lax.rsqrt(jnp.mean(rows * rows, axis=-1, keepdims=True) + epsilon)
            term = refs[nt + k][m].astype(jnp.float32) * (rows * inverse)
            total = term if total is None else total + term
        refs[2 * nt][m] = jnp.sum(total, axis=0, keepdims=True)


def weight_kernel(count, *refs):
    left = jnp.concatenate([r[0] for r in refs[:count]], axis=0)
    right = jnp.concatenate([r[0] for r in refs[count:-1]], axis=0)
    total = lax.dot_general(left, right, ROWS, preferred_element_type=jnp.float32)
    refs[-1][0] = total.astype(jnp.bfloat16)


def call(kernel, inputs, outs, flops):
    whole = pl.BlockSpec(memory_space=pltpu.VMEM)
    moved = sum(math.prod(a.shape) * a.dtype.itemsize for a in [*inputs, *outs])
    return pl.pallas_call(
        kernel,
        out_shape=outs,
        in_specs=[whole] * len(inputs),
        out_specs=[whole] * len(outs),
        cost_estimate=pl.CostEstimate(flops=flops, bytes_accessed=moved, transcendentals=0),
        compiler_params=pltpu.CompilerParams(vmem_limit_bytes=VMEM_BYTES),
    )(*inputs)


def weight_grad(lefts, rights, split_left):
    members, _, high = lefts[0].shape
    wide = rights[0].shape[2]
    depth = sum(a.shape[1] for a in lefts)
    extent = high if split_left else wide
    tile = 640 if extent % 640 == 0 else extent
    rows = lambda a: a.shape[1]
    if split_left:
        left = [pl.BlockSpec((1, rows(a), tile), lambda m, i: (m, 0, i)) for a in lefts]
        right = [pl.BlockSpec((1, rows(a), wide), lambda m, i: (m, 0, 0)) for a in rights]
        out = pl.BlockSpec((1, tile, wide), lambda m, i: (m, i, 0))
    else:
        left = [pl.BlockSpec((1, rows(a), high), lambda m, i: (m, 0, 0)) for a in lefts]
        right = [pl.BlockSpec((1, rows(a), tile), lambda m, i: (m, 0, i)) for a in rights]
        out = pl.BlockSpec((1, high, tile), lambda m, i: (m, 0, i))
    return pl.pallas_call(
        functools.partial(weight_kernel, len(lefts)),
        grid=(members, extent // tile),
        out_shape=jax.ShapeDtypeStruct((members, high, wide), jnp.bfloat16),
        in_specs=[*left, *right],
        out_specs=out,
        cost_estimate=pl.CostEstimate(
            flops=2 * members * depth * high * wide,
            bytes_accessed=2 * members * (depth * (high + wide) + high * wide),
            transcendentals=0,
        ),
        compiler_params=pltpu.CompilerParams(vmem_limit_bytes=VMEM_BYTES),
    )(*lefts, *rights)


def shift(value, axis, steps):
    count = lax.axis_size(axis)
    return lax.ppermute(value, axis, [(i, (i + steps) % count) for i in range(count)])


def sum_over(value, axis):
    count = lax.axis_size(axis)
    if count & (count - 1):
        return lax.psum(value, axis)
    terms = [value] + [
        lax.ppermute(value, axis, [(i, i ^ step) for i in range(count)]) for step in range(1, count)
    ]
    while len(terms) > 1:
        terms = [terms[i] + terms[i + 1] for i in range(0, len(terms), 2)]
    return terms[0]


def local(layer_in, carry_in, top_grad, w_qkv, w_out, gain):
    ticks = layer_in.shape[0]
    own_rows = layer_in.shape[4]
    width = layer_in.shape[5]
    nt = lax.axis_size("tensor")
    ns = lax.axis_size("section")
    nd = lax.axis_size("dp")
    length = own_rows * nt
    section = lax.axis_index("section")
    place = lax.axis_index("tensor")
    replica = lax.axis_index("dp")
    at_first = section == 0
    at_last = section == ns - 1
    x_rows = layer_in[:, :, 0, 0]
    carried = carry_in[:, 0, 0]
    fresh_rows = top_grad[:, 0]
    weight_qkv = [w_qkv[m, 0] for m in range(2)]
    weight_out = [w_out[m, 0] for m in range(2)]
    qkv_width = w_qkv.shape[3]
    head_width = w_out.shape[2]
    kv_local = qkv_width // ((GROUP + 2) * HD)
    bf16, f32 = jnp.bfloat16, jnp.float32

    block = jnp.arange(length) // own_rows
    positions = lax.rem(place - block + nt, nt) * own_rows + lax.rem(jnp.arange(length), own_rows)
    lanes = jnp.arange(2 * HD)
    frequency = rope_base ** (-((lanes % (HD // 2)).astype(f32) * (2.0 / HD)))
    angle = positions.astype(f32)[:, None] * frequency[None, :]
    cosine = jnp.cos(angle)
    sine = jnp.where(lanes[None, :] % HD < HD // 2, -jnp.sin(angle), jnp.sin(angle))
    bias = jnp.where(positions[:, None] >= positions[None, :], 0.0, -1e30).astype(f32)

    def gather_rotated(value):
        values = value if isinstance(value, list) else [value] * nt
        parts = [values[0]]
        for k in range(1, nt):
            parts.append(shift(values[k], "tensor", k))
        return parts

    def normalize(rows):
        rows = rows.astype(f32)
        inverse = lax.rsqrt(jnp.mean(rows * rows, axis=-1, keepdims=True) + epsilon)
        return rows * inverse, inverse

    def slice_for(value, p):
        extent = value.shape[2] // nd
        return lax.dynamic_slice_in_dim(value, ((replica + p) % nd) * extent, extent, axis=2)

    def peers(value, columns):
        return [shift(slice_for(value, p) if columns else value, "dp", p) for p in range(1, nd)]

    def send_parts(parts):
        sent = []
        for part in parts:
            sent.append(peers(part, False))
        return sent

    def shaped(*shape, dtype=bf16):
        return jax.ShapeDtypeStruct((2,) + shape, dtype)

    def forward(parts):
        return call(
            functools.partial(forward_kernel, nt, kv_local),
            [*parts, gain[:, 0:1], *weight_qkv, cosine, sine, bias],
            [
                shaped(length, width),
                shaped(length, head_width),
                shaped(length, qkv_width),
                shaped(length, kv_local * GROUP * length, dtype=f32),
            ],
            4 * length * width * qkv_width,
        )

    def backward(parts, rotated, softmax):
        outs = call(
            functools.partial(backward_kernel, nt, kv_local),
            [*parts, *weight_out, *weight_qkv, rotated, softmax, cosine, sine],
            [shaped(length, qkv_width)] + [shaped(own_rows, width)] * nt,
            4 * length * width * (qkv_width + head_width),
        )
        return outs[0], outs[1:]

    x_parts = gather_rotated(x_rows[0])
    own_grads = carried
    grad_parts = gather_rotated(carried)
    normed, attended, rotated, softmax = forward(x_parts)
    normed_peers = peers(normed, True)
    attended_peers = peers(attended, True)
    sent_parts = send_parts(grad_parts)
    qkv_lefts, qkv_rights, out_lefts, out_rights = [], [], [], []
    gain_total = 0.0
    per_tick = []
    for t in range(ticks):
        projected, partials = backward(grad_parts, rotated, softmax)
        received = []
        for k in range(1, nt):
            received.append(shift(partials[k], "tensor", -k))
        grad_peers = sent_parts
        projected_peers = peers(projected, False)
        gain_total = gain_total + call(
            functools.partial(gain_kernel, nt),
            [*x_parts, *partials],
            [shaped(1, width, dtype=f32)],
            2 * length * width,
        )[0]
        total = partials[0].astype(f32)
        for part in received:
            total = total + part.astype(f32)
        unit_own, inverse = normalize(x_rows[t])
        grad_unit = total * gain[:, 0:1]
        grad_rows = inverse * (
            grad_unit - unit_own * jnp.mean(grad_unit * unit_own, axis=-1, keepdims=True)
        )
        outcome = (own_grads.astype(f32) + grad_rows).astype(bf16)
        per_tick.append(outcome)
        qkv_lefts.extend([slice_for(normed, 0), *normed_peers])
        qkv_rights.extend([projected, *projected_peers])
        out_lefts.extend([slice_for(attended, 0), *attended_peers])
        out_rights.extend(grad_parts)
        for p in range(nd - 1):
            out_rights.extend(g[p] for g in grad_peers)
        if t + 1 < ticks:
            upward = lax.ppermute(outcome[1], "section", [(s, s + 1) for s in range(ns - 1)])
            downward = lax.ppermute(outcome[0], "section", [(s, s - 1) for s in range(1, ns)])
            own_grads = jnp.stack(
                [
                    jnp.where(at_last, outcome[1], downward),
                    jnp.where(at_first, fresh_rows[t], upward),
                ]
            )
            beside, _ = lax.optimization_barrier((x_rows[t + 1], grad_parts))
            later, _ = lax.optimization_barrier((x_rows[t + 1], received))
            x_parts = gather_rotated([beside if k == nt // 2 else later for k in range(nt)])
            grad_parts = gather_rotated(own_grads)
            normed, attended, rotated, softmax = forward(x_parts)
            normed_peers = peers(normed, True)
            attended_peers = peers(attended, True)
            sent_parts = send_parts(grad_parts)
            grad_parts, qkv_lefts, qkv_rights, out_lefts, out_rights = lax.optimization_barrier(
                (grad_parts, qkv_lefts, qkv_rights, out_lefts, out_rights)
            )

    grad_out = weight_grad(out_lefts, out_rights, False)
    grad_qkv = weight_grad(qkv_lefts, qkv_rights, True)
    for axis in ("dp", "tensor"):
        gain_total = sum_over(gain_total, axis)
    return (
        jnp.stack(per_tick)[:, :, None, None],
        grad_qkv[:, None],
        grad_out[:, None],
        gain_total,
    )


def solution(mesh):
    in_specs = (
        P(None, None, "section", "dp", "tensor", None),
        P(None, "section", "dp", "tensor", None),
        P(None, "dp", "tensor", None),
        P(None, "section", None, "tensor"),
        P(None, "section", "tensor", None),
        P(None, "section", None),
    )
    out_specs = (
        P(None, None, "section", "dp", "tensor", None),
        P(None, "section", "dp", "tensor"),
        P(None, "section", ("tensor", "dp"), None),
        P(None, "section", None),
    )

    return jax.shard_map(local, mesh=mesh, in_specs=in_specs, out_specs=out_specs, check_vma=False)
```

```python
import functools
import math

import jax
import jax.numpy as jnp
from jax import lax
from jax.experimental import pallas as pl
from jax.experimental.pallas import tpu as pltpu
from jax.sharding import PartitionSpec as P


HD = 64
GROUP = 8

epsilon = 1e-06
rope_base = 1000000.0


ROWS = (((0,), (0,)), ((), ()))
COLS = (((1,), (1,)), ((), ()))
VMEM_BYTES = 8 * 1024 * 1024


def swap_halves(values, lane):
    width = values.shape[-1]
    half = HD // 2
    ahead = pltpu.roll(values, width - half, 1)
    behind = pltpu.roll(values, half, 1)
    return jnp.where(lane % HD < half, ahead, behind)


def pair_up(values, lane):
    low = jnp.where(lane < HD, values, 0.0)
    high = pltpu.roll(low, HD, 1)
    return jnp.concatenate([low, high], axis=0).astype(jnp.bfloat16)


def pick(parts, nt, flag_ref, m):
    blocks = [p[m] if len(p.shape) == 3 else p[...] for p in parts]
    if len(parts) > nt:
        far = blocks.pop()
        blocks[1] = jnp.where(flag_ref[0] == 0, far, blocks[1])
        blocks[nt - 1] = jnp.where(flag_ref[0] == nt - 1, far, blocks[nt - 1])
    return blocks


def forward_kernel(nt, given, kv_local, flag_ref, *refs):
    parts, rest = refs[:given], refs[given:]
    gain_ref, *weight_refs, cos_ref, sin_ref, bias_ref = rest[:6]
    normed_ref, attended_ref, rotated_ref, softmax_ref = rest[6:]
    cosine, sine, bias = cos_ref[...], sin_ref[...], bias_ref[...]
    scale = 1.0 / math.sqrt(HD)
    chunks = GROUP // 2
    for m in range(2):
        blocks = pick(parts, nt, flag_ref, m)
        rows = jnp.concatenate([b.astype(jnp.float32) for b in blocks], axis=0)
        inverse = lax.rsqrt(jnp.mean(rows * rows, axis=-1, keepdims=True) + epsilon)
        normed = (rows * inverse * gain_ref[m]).astype(jnp.bfloat16)
        normed_ref[m] = normed
        projected = jnp.dot(normed, weight_refs[m][...], preferred_element_type=jnp.float32)
        length = rows.shape[0]
        lane = lax.broadcasted_iota(jnp.int32, (length, 2 * HD), 1)
        for group in range(kv_local):
            base = group * (GROUP + 2) * HD
            at = base + GROUP * HD
            pair = projected[:, at : at + 2 * HD]
            turned = pair * cosine + swap_halves(pair, lane) * sine
            key_value = jnp.where(lane < HD, turned, pair)
            rotated_ref[m, :, at : at + 2 * HD] = key_value.astype(jnp.bfloat16)
            keys = pair_up(key_value, lane)
            values = pair_up(pltpu.roll(key_value, HD, 1), lane)
            for c in range(chunks):
                lo = base + c * 2 * HD
                heads = projected[:, lo : lo + 2 * HD]
                query = (heads * cosine + swap_halves(heads, lane) * sine).astype(jnp.bfloat16)
                rotated_ref[m, :, lo : lo + 2 * HD] = query
                scores = lax.dot_general(query, keys, COLS, preferred_element_type=jnp.float32)
                softmax = []
                for h in range(2):
                    one = scores[:, h * length : (h + 1) * length] * scale + bias
                    power = jnp.exp(one - jnp.max(one, axis=-1, keepdims=True))
                    softmax.append(power / jnp.sum(power, axis=-1, keepdims=True))
                softmax = jnp.concatenate(softmax, axis=1)
                so = (group * chunks + c) * 2 * length
                softmax_ref[m, :, so : so + 2 * length] = softmax
                attended = jnp.dot(
                    softmax.astype(jnp.bfloat16), values, preferred_element_type=jnp.float32
                )
                ao = (group * chunks + c) * 2 * HD
                attended_ref[m, :, ao : ao + 2 * HD] = attended.astype(jnp.bfloat16)


def backward_kernel(nt, given, kv_local, m, flag_ref, *refs):
    parts, rest = refs[:given], refs[given:]
    wout_ref, wqkv_ref, rotated_ref, softmax_ref, cos_ref, sin_ref = rest[:6]
    projected_ref = rest[-nt - 1]
    partial_refs = rest[-nt:]
    own = parts[0].shape[-2]
    length = own * nt
    lane = lax.broadcasted_iota(jnp.int32, (length, 2 * HD), 1)
    cosine, sine = cos_ref[...], sin_ref[...]
    scale = 1.0 / math.sqrt(HD)
    chunks = GROUP // 2

    def unturn(values):
        return values * cosine - swap_halves(values, lane) * sine

    grad_full = jnp.concatenate(pick(parts, nt, flag_ref, m), axis=0)
    grad_attended = lax.dot_general(
        grad_full, wout_ref[...], COLS, preferred_element_type=jnp.float32
    ).astype(jnp.bfloat16)
    for group in range(kv_local):
        base = group * (GROUP + 2) * HD
        at = base + GROUP * HD
        key_value = rotated_ref[m, :, at : at + 2 * HD].astype(jnp.float32)
        keys = pair_up(key_value, lane)
        values = pair_up(pltpu.roll(key_value, HD, 1), lane)
        key_sum = jnp.zeros((2 * length, 2 * HD), jnp.float32)
        value_sum = jnp.zeros((2 * length, 2 * HD), jnp.float32)
        for c in range(chunks):
            lo = base + c * 2 * HD
            ao = (group * chunks + c) * 2 * HD
            so = (group * chunks + c) * 2 * length
            grad_heads = grad_attended[:, ao : ao + 2 * HD]
            softmax = softmax_ref[m, :, so : so + 2 * length]
            grad_softmax = lax.dot_general(
                grad_heads, values, COLS, preferred_element_type=jnp.float32
            )
            grad_scores = []
            for h in range(2):
                here = slice(h * length, (h + 1) * length)
                sm, gs = softmax[:, here], grad_softmax[:, here]
                total = jnp.sum(sm * gs, axis=-1, keepdims=True)
                grad_scores.append((sm * (gs - total) * scale).astype(jnp.bfloat16))
            grad_scores = jnp.concatenate(grad_scores, axis=1)
            grad_query = jnp.dot(grad_scores, keys, preferred_element_type=jnp.float32)
            projected_ref[:, lo : lo + 2 * HD] = unturn(grad_query).astype(jnp.bfloat16)
            query = rotated_ref[m, :, lo : lo + 2 * HD]
            key_sum = key_sum + lax.dot_general(
                grad_scores, query, ROWS, preferred_element_type=jnp.float32
            )
            value_sum = value_sum + lax.dot_general(
                softmax.astype(jnp.bfloat16),
                grad_heads,
                ROWS,
                preferred_element_type=jnp.float32,
            )
        grad_key = unturn(key_sum[:length] + pltpu.roll(key_sum[length:], HD, 1))
        grad_value = pltpu.roll(value_sum[:length], HD, 1) + value_sum[length:]
        projected_ref[:, at : at + 2 * HD] = jnp.where(
            lane < HD, grad_key, grad_value
        ).astype(jnp.bfloat16)
    partial = lax.dot_general(
        projected_ref[...], wqkv_ref[...], COLS, preferred_element_type=jnp.float32
    ).astype(jnp.bfloat16)
    for k in range(nt):
        partial_refs[k][...] = partial[k * own : (k + 1) * own]


def choose_kernel(flag, where_ref, chosen_ref, otherwise_ref, out_ref):
    out_ref[...] = jnp.where(where_ref[flag] == 1, chosen_ref[...], otherwise_ref[...])


def norm_kernel(m, _, x_ref, grad_ref, gain_ref, *refs):
    grad_normed = refs[0][...].astype(jnp.float32)
    for ref in refs[1:-1]:
        grad_normed = grad_normed + ref[...].astype(jnp.float32)
    rows = x_ref[m].astype(jnp.float32)
    inverse = lax.rsqrt(jnp.mean(rows * rows, axis=-1, keepdims=True) + epsilon)
    unit = rows * inverse
    grad_unit = grad_normed * gain_ref[m]
    grad_rows = inverse * (
        grad_unit - unit * jnp.mean(grad_unit * unit, axis=-1, keepdims=True)
    )
    refs[-1][...] = (grad_ref[...].astype(jnp.float32) + grad_rows).astype(jnp.bfloat16)


def gain_kernel(nt, given, flag_ref, *refs):
    parts, partials, out_ref = refs[:given], refs[given:-1], refs[-1]
    for m in range(2):
        total = None
        for k, block in enumerate(pick(parts, nt, flag_ref, m)):
            rows = block.astype(jnp.float32)
            inverse = lax.rsqrt(jnp.mean(rows * rows, axis=-1, keepdims=True) + epsilon)
            term = partials[m * nt + k][...].astype(jnp.float32) * (rows * inverse)
            total = term if total is None else total + term
        out_ref[m] = jnp.sum(total, axis=0, keepdims=True)


def weight_kernel(count, rights, *refs):
    def joined(some):
        return jnp.concatenate([r[0] if len(r.shape) == 3 else r[...] for r in some], axis=0)

    total = lax.dot_general(
        joined(refs[:count]),
        joined(refs[count : count + rights]),
        ROWS,
        preferred_element_type=jnp.float32,
    )
    refs[-1][0] = total.astype(jnp.bfloat16)


def call(kernel, inputs, outs, flops):
    whole = pl.BlockSpec(memory_space=pltpu.VMEM)
    moved = sum(math.prod(a.shape) * a.dtype.itemsize for a in [*inputs, *outs])
    return pl.pallas_call(
        kernel,
        out_shape=outs,
        in_specs=[pl.BlockSpec(memory_space=pltpu.SMEM)] + [whole] * (len(inputs) - 1),
        out_specs=[whole] * len(outs),
        cost_estimate=pl.CostEstimate(flops=flops, bytes_accessed=moved, transcendentals=0),
        compiler_params=pltpu.CompilerParams(vmem_limit_bytes=VMEM_BYTES),
    )(*inputs)


def weight_grad(lefts, rights, split_left, only=None, earlier=None):
    members = 2
    depth = sum(a.shape[-2] for a in lefts)
    high, wide = lefts[0].shape[-1], rights[0].shape[-1]
    extent = high if split_left else wide
    tile = 640 if extent % 640 == 0 else extent

    def member(m):
        return m if only is None else only

    def spec(a, tiled):
        rows, columns = a.shape[-2], tile if tiled else a.shape[-1]
        if len(a.shape) == 3:
            return pl.BlockSpec(
                (1, rows, columns), lambda m, i: (member(m), 0, i if tiled else 0)
            )
        return pl.BlockSpec((rows, columns), lambda m, i: (0, i if tiled else 0))

    specs = [spec(a, split_left) for a in lefts] + [spec(a, not split_left) for a in rights]
    inputs = [*lefts, *rights]
    aliases = {}
    if earlier is not None:
        aliases = {len(inputs): 0}
        inputs.append(earlier)
        specs.append(pl.BlockSpec(memory_space=pl.ANY))
    if split_left:
        out = pl.BlockSpec((1, tile, wide), lambda m, i: (member(m), i, 0))
    else:
        out = pl.BlockSpec((1, high, tile), lambda m, i: (member(m), 0, i))
    count = members if only is None else 1
    return pl.pallas_call(
        functools.partial(weight_kernel, len(lefts), len(rights)),
        grid=(count, extent // tile),
        out_shape=jax.ShapeDtypeStruct((members, high, wide), jnp.bfloat16),
        in_specs=specs,
        out_specs=out,
        input_output_aliases=aliases,
        cost_estimate=pl.CostEstimate(
            flops=2 * count * depth * high * wide,
            bytes_accessed=2 * count * (depth * (high + wide) + high * wide),
            transcendentals=0,
        ),
        compiler_params=pltpu.CompilerParams(vmem_limit_bytes=VMEM_BYTES),
    )(*inputs)


def shift(value, axis, steps):
    count = lax.axis_size(axis)
    return lax.ppermute(value, axis, [(i, (i + steps) % count) for i in range(count)])


def sum_over(value, axis):
    count = lax.axis_size(axis)
    if count & (count - 1):
        return lax.psum(value, axis)
    terms = [value] + [
        lax.ppermute(value, axis, [(i, i ^ step) for i in range(count)]) for step in range(1, count)
    ]
    while len(terms) > 1:
        terms = [terms[i] + terms[i + 1] for i in range(0, len(terms), 2)]
    return terms[0]


def local(layer_in, carry_in, top_grad, w_qkv, w_out, gain):
    ticks = layer_in.shape[0]
    own_rows = layer_in.shape[4]
    width = layer_in.shape[5]
    nt = lax.axis_size("tensor")
    ns = lax.axis_size("section")
    nd = lax.axis_size("dp")
    length = own_rows * nt
    section = lax.axis_index("section")
    place = lax.axis_index("tensor")
    replica = lax.axis_index("dp")
    at_first = section == 0
    at_last = section == ns - 1
    at_far_low, at_far_high = place == 0, place == nt - 1
    x_rows = layer_in[:, :, 0, 0]
    carried = carry_in[:, 0, 0]
    fresh_rows = top_grad[:, 0]
    weight_qkv = [w_qkv[m, 0] for m in range(2)]
    weight_out = [w_out[m, 0] for m in range(2)]
    qkv_width = w_qkv.shape[3]
    head_width = w_out.shape[2]
    kv_local = qkv_width // ((GROUP + 2) * HD)
    bf16, f32 = jnp.bfloat16, jnp.float32

    block = jnp.arange(length) // own_rows
    positions = lax.rem(place - block + nt, nt) * own_rows + lax.rem(jnp.arange(length), own_rows)
    lanes = jnp.arange(2 * HD)
    frequency = rope_base ** (-((lanes % (HD // 2)).astype(f32) * (2.0 / HD)))
    angle = positions.astype(f32)[:, None] * frequency[None, :]
    cosine = jnp.cos(angle)
    sine = jnp.where(lanes[None, :] % HD < HD // 2, -jnp.sin(angle), jnp.sin(angle))
    bias = jnp.where(positions[:, None] >= positions[None, :], 0.0, -1e30).astype(f32)

    def gather_rotated(value):
        parts = [value]
        for k in range(1, nt):
            parts.append(shift(value, "tensor", k))
        return parts

    def gather_line(near, far):
        if nt != 4:
            return gather_rotated(near)
        middle = shift(far, "tensor", 2)
        ahead = lax.ppermute(near, "tensor", [(i, i + 1) for i in range(nt - 1)])
        behind = lax.ppermute(near, "tensor", [(i, i - 1) for i in range(1, nt)])
        ends = lax.ppermute(middle, "tensor", [(1, 0), (nt - 2, nt - 1)])
        return [near, ahead, middle, behind, ends]

    def slice_for(value, p):
        extent = value.shape[2] // nd
        return lax.dynamic_slice_in_dim(value, ((replica + p) % nd) * extent, extent, axis=2)

    def peers(value, columns):
        return [shift(slice_for(value, p) if columns else value, "dp", p) for p in range(1, nd)]

    def send_parts(parts):
        sent = []
        for part in parts:
            sent.append(peers(part, False))
        return sent

    def shaped(*shape, dtype=bf16):
        return jax.ShapeDtypeStruct((2,) + shape, dtype)

    where = jnp.stack([place, at_last, at_first, at_far_low, at_far_high]).astype(jnp.int32)

    def choose(flag, chosen, otherwise):
        return call(
            functools.partial(choose_kernel, flag),
            [where, chosen, otherwise],
            [jax.ShapeDtypeStruct(otherwise.shape, bf16)],
            own_rows * width,
        )[0]


    def settled(parts):
        if len(parts) == nt:
            return parts
        parts, ends = list(parts[:nt]), parts[nt]
        parts[1] = choose(3, ends, parts[1])
        parts[nt - 1] = choose(4, ends, parts[nt - 1])
        return parts

    def forward(parts):
        return call(
            functools.partial(forward_kernel, nt, len(parts), kv_local),
            [where, *parts, gain[:, 0:1], *weight_qkv, cosine, sine, bias],
            [
                shaped(length, width),
                shaped(length, head_width),
                shaped(length, qkv_width),
                shaped(length, kv_local * GROUP * length, dtype=f32),
            ],
            4 * length * width * qkv_width,
        )

    def backward(parts, m, rotated, softmax):
        outs = call(
            functools.partial(backward_kernel, nt, len(parts), kv_local, m),
            [where, *parts, weight_out[m], weight_qkv[m], rotated, softmax, cosine, sine],
            [jax.ShapeDtypeStruct((length, qkv_width), bf16)]
            + [jax.ShapeDtypeStruct((own_rows, width), bf16)] * nt,
            2 * length * width * (qkv_width + head_width),
        )
        return outs[0], outs[1:]

    members = (1, 0)
    x_parts = gather_rotated(x_rows[0])
    own_grads = [carried[0], carried[1]]
    first_parts = gather_line(carried, carried)
    grad_parts = [first_parts, first_parts]
    normed, attended, rotated, softmax = forward(x_parts)
    normed_peers = peers(normed, True)
    attended_peers = peers(attended, True)
    placed = settled(first_parts)
    shared = send_parts(placed)
    placed, sent_parts = [placed, placed], [shared, shared]
    qkv_lefts, qkv_rights, out_lefts, out_rights = [], [], [], [[], []]
    gain_total = 0.0
    per_tick = []
    for t in range(ticks):
        projected = [None, None]
        partials, received = [None, None], [[], []]
        for m in members:
            projected[m], partials[m] = backward(grad_parts[m], m, rotated, softmax)
            for k in range(1, nt):
                received[m].append(shift(partials[m][k], "tensor", -k))
        projected = jnp.stack(projected)
        projected_peers = peers(projected, False)
        gain_total = gain_total + call(
            functools.partial(gain_kernel, nt, len(x_parts)),
            [where, *x_parts, *partials[0], *partials[1]],
            [shaped(1, width, dtype=f32)],
            2 * length * width,
        )[0]
        outcome = [None, None]
        for m in members:
            outcome[m] = call(
                functools.partial(norm_kernel, m),
                [where, x_parts[0], own_grads[m], gain[:, 0:1], partials[m][0], *received[m]],
                [jax.ShapeDtypeStruct((own_rows, width), bf16)],
                own_rows * width,
            )[0]
        per_tick.append(jnp.stack(outcome))
        qkv_lefts.extend([slice_for(normed, 0), *normed_peers])
        qkv_rights.extend([projected, *projected_peers])
        out_lefts.extend([slice_for(attended, 0), *attended_peers])
        for m in members:
            out_rights[m].extend(placed[m])
            for p in range(nd - 1):
                out_rights[m].extend(g[p] for g in sent_parts[m])
        if t + 1 < ticks:
            later = x_rows[t + 1]
            if t > 0:
                later, _ = lax.optimization_barrier((later, received))
            x_parts = gather_line(later, later)
            normed, attended, rotated, softmax = forward(x_parts)
            normed_peers = peers(normed, True)
            attended_peers = peers(attended, True)
            own_grads, grad_parts, sent_parts = [None, None], [None, None], [None, None]
            for m in members:
                if m == 1:
                    moves = [(s, s + 1) for s in range(ns - 1)]
                    came = lax.ppermute(outcome[1], "section", moves)
                    own_grads[1] = choose(2, fresh_rows[t], came)
                else:
                    moves = [(s, s - 1) for s in range(1, ns)]
                    came = lax.ppermute(outcome[0], "section", moves)
                    own_grads[0] = choose(1, outcome[1], came)
                grad_parts[m] = gather_rotated(own_grads[m])
                sent_parts[m] = send_parts(grad_parts[m])
            placed = grad_parts

    grad_out = None
    for m in members:
        grad_out = weight_grad(out_lefts, out_rights[m], False, m, grad_out)
    grad_qkv = weight_grad(qkv_lefts, qkv_rights, True)
    for axis in ("dp", "tensor"):
        gain_total = sum_over(gain_total, axis)
    return (
        jnp.stack(per_tick)[:, :, None, None],
        grad_qkv[:, None],
        grad_out[:, None],
        gain_total,
    )


def solution(mesh):
    in_specs = (
        P(None, None, "section", "dp", "tensor", None),
        P(None, "section", "dp", "tensor", None),
        P(None, "dp", "tensor", None),
        P(None, "section", None, "tensor"),
        P(None, "section", "tensor", None),
        P(None, "section", None),
    )
    out_specs = (
        P(None, None, "section", "dp", "tensor", None),
        P(None, "section", "dp", "tensor"),
        P(None, "section", ("tensor", "dp"), None),
        P(None, "section", None),
    )

    return jax.shard_map(local, mesh=mesh, in_specs=in_specs, out_specs=out_specs, check_vma=False)
```

```python
import functools
import math

import jax
import jax.numpy as jnp
from jax import lax
from jax.experimental import pallas as pl
from jax.experimental.pallas import tpu as pltpu
from jax.sharding import PartitionSpec as P


HD = 64
GROUP = 8

epsilon = 1e-06
rope_base = 1000000.0


ROWS = (((0,), (0,)), ((), ()))
COLS = (((1,), (1,)), ((), ()))
VMEM_BYTES = 16 * 1024 * 1024


def swap_halves(values, lane):
    width = values.shape[-1]
    half = HD // 2
    ahead = pltpu.roll(values, width - half, 1)
    behind = pltpu.roll(values, half, 1)
    return jnp.where(lane % HD < half, ahead, behind)


def pair_up(values, lane):
    low = jnp.where(lane < HD, values, 0.0)
    high = pltpu.roll(low, HD, 1)
    return jnp.concatenate([low, high], axis=0).astype(jnp.bfloat16)


def pick(parts, nt, flag_ref, m):
    blocks = [p[m] if len(p.shape) == 3 else p[...] for p in parts]
    if len(parts) > nt:
        far = blocks.pop()
        blocks[1] = jnp.where(flag_ref[0] == 0, far, blocks[1])
        blocks[nt - 1] = jnp.where(flag_ref[0] == nt - 1, far, blocks[nt - 1])
    return blocks


def forward_kernel(nt, given, kv_local, flag_ref, *refs):
    parts, rest = refs[:given], refs[given:]
    gain_ref, *weight_refs, cos_ref, sin_ref, bias_ref = rest[:6]
    normed_ref, attended_ref, rotated_ref, softmax_ref = rest[6:]
    cosine, sine, bias = cos_ref[...], sin_ref[...], bias_ref[...]
    scale = 1.0 / math.sqrt(HD)
    chunks = GROUP // 2
    for m in range(2):
        blocks = pick(parts, nt, flag_ref, m)
        rows = jnp.concatenate([b.astype(jnp.float32) for b in blocks], axis=0)
        inverse = lax.rsqrt(jnp.mean(rows * rows, axis=-1, keepdims=True) + epsilon)
        normed = (rows * inverse * gain_ref[m]).astype(jnp.bfloat16)
        normed_ref[m] = normed
        projected = jnp.dot(normed, weight_refs[m][...], preferred_element_type=jnp.float32)
        length = rows.shape[0]
        lane = lax.broadcasted_iota(jnp.int32, (length, 2 * HD), 1)
        for group in range(kv_local):
            base = group * (GROUP + 2) * HD
            at = base + GROUP * HD
            pair = projected[:, at : at + 2 * HD]
            turned = pair * cosine + swap_halves(pair, lane) * sine
            key_value = jnp.where(lane < HD, turned, pair)
            rotated_ref[m, :, at : at + 2 * HD] = key_value.astype(jnp.bfloat16)
            keys = pair_up(key_value, lane)
            values = pair_up(pltpu.roll(key_value, HD, 1), lane)
            for c in range(chunks):
                lo = base + c * 2 * HD
                heads = projected[:, lo : lo + 2 * HD]
                query = (heads * cosine + swap_halves(heads, lane) * sine).astype(jnp.bfloat16)
                rotated_ref[m, :, lo : lo + 2 * HD] = query
                scores = lax.dot_general(query, keys, COLS, preferred_element_type=jnp.float32)
                softmax = []
                for h in range(2):
                    one = scores[:, h * length : (h + 1) * length] * scale + bias
                    power = jnp.exp(one - jnp.max(one, axis=-1, keepdims=True))
                    softmax.append(power / jnp.sum(power, axis=-1, keepdims=True))
                softmax = jnp.concatenate(softmax, axis=1)
                so = (group * chunks + c) * 2 * length
                softmax_ref[m, :, so : so + 2 * length] = softmax
                attended = jnp.dot(
                    softmax.astype(jnp.bfloat16), values, preferred_element_type=jnp.float32
                )
                ao = (group * chunks + c) * 2 * HD
                attended_ref[m, :, ao : ao + 2 * HD] = attended.astype(jnp.bfloat16)


def backward_kernel(nt, given, kv_local, m, flag_ref, *refs):
    parts, rest = refs[:given], refs[given:]
    wout_ref, wqkv_ref, rotated_ref, softmax_ref, cos_ref, sin_ref = rest[:6]
    projected_ref = rest[-nt - 1]
    partial_refs = rest[-nt:]
    own = parts[0].shape[-2]
    length = own * nt
    lane = lax.broadcasted_iota(jnp.int32, (length, 2 * HD), 1)
    cosine, sine = cos_ref[...], sin_ref[...]
    scale = 1.0 / math.sqrt(HD)
    chunks = GROUP // 2

    def unturn(values):
        return values * cosine - swap_halves(values, lane) * sine

    grad_full = jnp.concatenate(pick(parts, nt, flag_ref, m), axis=0)
    grad_attended = lax.dot_general(
        grad_full, wout_ref[...], COLS, preferred_element_type=jnp.float32
    ).astype(jnp.bfloat16)
    for group in range(kv_local):
        base = group * (GROUP + 2) * HD
        at = base + GROUP * HD
        key_value = rotated_ref[m, :, at : at + 2 * HD].astype(jnp.float32)
        keys = pair_up(key_value, lane)
        values = pair_up(pltpu.roll(key_value, HD, 1), lane)
        key_sum = jnp.zeros((2 * length, 2 * HD), jnp.float32)
        value_sum = jnp.zeros((2 * length, 2 * HD), jnp.float32)
        for c in range(chunks):
            lo = base + c * 2 * HD
            ao = (group * chunks + c) * 2 * HD
            so = (group * chunks + c) * 2 * length
            grad_heads = grad_attended[:, ao : ao + 2 * HD]
            softmax = softmax_ref[m, :, so : so + 2 * length]
            grad_softmax = lax.dot_general(
                grad_heads, values, COLS, preferred_element_type=jnp.float32
            )
            grad_scores = []
            for h in range(2):
                here = slice(h * length, (h + 1) * length)
                sm, gs = softmax[:, here], grad_softmax[:, here]
                total = jnp.sum(sm * gs, axis=-1, keepdims=True)
                grad_scores.append((sm * (gs - total) * scale).astype(jnp.bfloat16))
            grad_scores = jnp.concatenate(grad_scores, axis=1)
            grad_query = jnp.dot(grad_scores, keys, preferred_element_type=jnp.float32)
            projected_ref[:, lo : lo + 2 * HD] = unturn(grad_query).astype(jnp.bfloat16)
            query = rotated_ref[m, :, lo : lo + 2 * HD]
            key_sum = key_sum + lax.dot_general(
                grad_scores, query, ROWS, preferred_element_type=jnp.float32
            )
            value_sum = value_sum + lax.dot_general(
                softmax.astype(jnp.bfloat16),
                grad_heads,
                ROWS,
                preferred_element_type=jnp.float32,
            )
        grad_key = unturn(key_sum[:length] + pltpu.roll(key_sum[length:], HD, 1))
        grad_value = pltpu.roll(value_sum[:length], HD, 1) + value_sum[length:]
        projected_ref[:, at : at + 2 * HD] = jnp.where(
            lane < HD, grad_key, grad_value
        ).astype(jnp.bfloat16)
    partial = lax.dot_general(
        projected_ref[...], wqkv_ref[...], COLS, preferred_element_type=jnp.float32
    ).astype(jnp.bfloat16)
    for k in range(nt):
        partial_refs[k][...] = partial[k * own : (k + 1) * own]


def join_kernel(nt, flag_ref, *refs):
    parts, out_ref = refs[:-1], refs[-1]
    own = parts[0].shape[-2]
    for m in range(out_ref.shape[0]) if len(out_ref.shape) == 3 else (None,):
        for k, block in enumerate(pick(parts, nt, flag_ref, m)[1:]):
            if m is None:
                out_ref[k * own : (k + 1) * own] = block
            else:
                out_ref[m, k * own : (k + 1) * own] = block


def choose_kernel(flag, where_ref, chosen_ref, otherwise_ref, out_ref):
    out_ref[...] = jnp.where(where_ref[flag] == 1, chosen_ref[...], otherwise_ref[...])


def norm_kernel(m, _, x_ref, grad_ref, gain_ref, *refs):
    grad_normed = refs[0][...].astype(jnp.float32)
    for ref in refs[1:-1]:
        grad_normed = grad_normed + ref[...].astype(jnp.float32)
    rows = x_ref[m].astype(jnp.float32)
    inverse = lax.rsqrt(jnp.mean(rows * rows, axis=-1, keepdims=True) + epsilon)
    unit = rows * inverse
    grad_unit = grad_normed * gain_ref[m]
    grad_rows = inverse * (
        grad_unit - unit * jnp.mean(grad_unit * unit, axis=-1, keepdims=True)
    )
    refs[-1][...] = (grad_ref[...].astype(jnp.float32) + grad_rows).astype(jnp.bfloat16)


def gain_kernel(nt, given, flag_ref, *refs):
    parts, partials, out_ref = refs[:given], refs[given:-1], refs[-1]
    for m in range(2):
        total = None
        for k, block in enumerate(pick(parts, nt, flag_ref, m)):
            rows = block.astype(jnp.float32)
            inverse = lax.rsqrt(jnp.mean(rows * rows, axis=-1, keepdims=True) + epsilon)
            term = partials[m * nt + k][...].astype(jnp.float32) * (rows * inverse)
            total = term if total is None else total + term
        out_ref[m] = jnp.sum(total, axis=0, keepdims=True)


def weight_kernel(count, rights, *refs):
    def joined(some):
        return jnp.concatenate([r[0] if len(r.shape) == 3 else r[...] for r in some], axis=0)

    total = lax.dot_general(
        joined(refs[:count]),
        joined(refs[count : count + rights]),
        ROWS,
        preferred_element_type=jnp.float32,
    )
    refs[-1][0] = total.astype(jnp.bfloat16)


def call(kernel, inputs, outs, flops):
    whole = pl.BlockSpec(memory_space=pltpu.VMEM)
    moved = sum(math.prod(a.shape) * a.dtype.itemsize for a in [*inputs, *outs])
    return pl.pallas_call(
        kernel,
        out_shape=outs,
        in_specs=[pl.BlockSpec(memory_space=pltpu.SMEM)] + [whole] * (len(inputs) - 1),
        out_specs=[whole] * len(outs),
        cost_estimate=pl.CostEstimate(flops=flops, bytes_accessed=moved, transcendentals=0),
        compiler_params=pltpu.CompilerParams(vmem_limit_bytes=VMEM_BYTES),
    )(*inputs)


def weight_grad(lefts, rights, split_left, only=None, earlier=None):
    members = 2
    depth = sum(a.shape[-2] for a in lefts)
    high, wide = lefts[0].shape[-1], rights[0].shape[-1]
    extent = high if split_left else wide
    tile = 1280 if extent % 1280 == 0 else extent

    def member(m):
        return m if only is None else only

    def spec(a, tiled):
        rows, columns = a.shape[-2], tile if tiled else a.shape[-1]
        if len(a.shape) == 3:
            return pl.BlockSpec(
                (1, rows, columns), lambda m, i: (member(m), 0, i if tiled else 0)
            )
        return pl.BlockSpec((rows, columns), lambda m, i: (0, i if tiled else 0))

    specs = [spec(a, split_left) for a in lefts] + [spec(a, not split_left) for a in rights]
    inputs = [*lefts, *rights]
    aliases = {}
    if earlier is not None:
        aliases = {len(inputs): 0}
        inputs.append(earlier)
        specs.append(pl.BlockSpec(memory_space=pl.ANY))
    if split_left:
        out = pl.BlockSpec((1, tile, wide), lambda m, i: (member(m), i, 0))
    else:
        out = pl.BlockSpec((1, high, tile), lambda m, i: (member(m), 0, i))
    count = members if only is None else 1
    return pl.pallas_call(
        functools.partial(weight_kernel, len(lefts), len(rights)),
        grid=(count, extent // tile),
        out_shape=jax.ShapeDtypeStruct((members, high, wide), jnp.bfloat16),
        in_specs=specs,
        out_specs=out,
        input_output_aliases=aliases,
        cost_estimate=pl.CostEstimate(
            flops=2 * count * depth * high * wide,
            bytes_accessed=2 * count * (depth * (high + wide) + high * wide),
            transcendentals=0,
        ),
        compiler_params=pltpu.CompilerParams(vmem_limit_bytes=VMEM_BYTES),
    )(*inputs)


def shift(value, axis, steps):
    count = lax.axis_size(axis)
    return lax.ppermute(value, axis, [(i, (i + steps) % count) for i in range(count)])


def sum_over(value, axis):
    count = lax.axis_size(axis)
    if count & (count - 1):
        return lax.psum(value, axis)
    step = 1
    while step < count:
        value = value + lax.ppermute(value, axis, [(i, i ^ step) for i in range(count)])
        step *= 2
    return value


def local(layer_in, carry_in, top_grad, w_qkv, w_out, gain):
    ticks = layer_in.shape[0]
    own_rows = layer_in.shape[4]
    width = layer_in.shape[5]
    nt = lax.axis_size("tensor")
    ns = lax.axis_size("section")
    nd = lax.axis_size("dp")
    length = own_rows * nt
    section = lax.axis_index("section")
    place = lax.axis_index("tensor")
    replica = lax.axis_index("dp")
    at_first = section == 0
    at_last = section == ns - 1
    x_rows = layer_in[:, :, 0, 0]
    carried = carry_in[:, 0, 0]
    fresh_rows = top_grad[:, 0]
    weight_qkv = [w_qkv[m, 0] for m in range(2)]
    weight_out = [w_out[m, 0] for m in range(2)]
    qkv_width = w_qkv.shape[3]
    head_width = w_out.shape[2]
    kv_local = qkv_width // ((GROUP + 2) * HD)
    bf16, f32 = jnp.bfloat16, jnp.float32

    block = jnp.arange(length) // own_rows
    positions = lax.rem(place - block + nt, nt) * own_rows + lax.rem(jnp.arange(length), own_rows)
    lanes = jnp.arange(2 * HD)
    frequency = rope_base ** (-((lanes % (HD // 2)).astype(f32) * (2.0 / HD)))
    angle = positions.astype(f32)[:, None] * frequency[None, :]
    cosine = jnp.cos(angle)
    sine = jnp.where(lanes[None, :] % HD < HD // 2, -jnp.sin(angle), jnp.sin(angle))
    bias = jnp.where(positions[:, None] >= positions[None, :], 0.0, -1e30).astype(f32)

    def gather_rotated(value):
        parts = [value]
        for k in range(1, nt):
            parts.append(shift(value, "tensor", k))
        return parts

    def gather_line(near, far):
        if nt != 4:
            return gather_rotated(near)
        middle = shift(far, "tensor", 2)
        ahead = lax.ppermute(near, "tensor", [(i, i + 1) for i in range(nt - 1)])
        behind = lax.ppermute(near, "tensor", [(i, i - 1) for i in range(1, nt)])
        ends = lax.ppermute(middle, "tensor", [(1, 0), (nt - 2, nt - 1)])
        return [near, ahead, middle, behind, ends]

    def slice_for(value, p):
        extent = value.shape[2] // nd
        return lax.dynamic_slice_in_dim(value, ((replica + p) % nd) * extent, extent, axis=2)

    def peers(value, columns):
        return [shift(slice_for(value, p) if columns else value, "dp", p) for p in range(1, nd)]

    def send_parts(parts):
        sent = []
        for part in parts:
            sent.append(peers(part, False))
        return sent

    def shaped(*shape, dtype=bf16):
        return jax.ShapeDtypeStruct((2,) + shape, dtype)

    where = jnp.stack([place, at_last, at_first]).astype(jnp.int32)

    def choose(flag, chosen, otherwise):
        return call(
            functools.partial(choose_kernel, flag),
            [where, chosen, otherwise],
            [jax.ShapeDtypeStruct(otherwise.shape, bf16)],
            own_rows * width,
        )[0]


    def settled(parts):
        shape = parts[0].shape[:-2] + (length - own_rows, width)
        others = call(
            functools.partial(join_kernel, nt),
            [where, *parts],
            [jax.ShapeDtypeStruct(shape, bf16)],
            length * width,
        )[0]
        return [parts[0], others]

    def forward(parts):
        return call(
            functools.partial(forward_kernel, nt, len(parts), kv_local),
            [where, *parts, gain[:, 0:1], *weight_qkv, cosine, sine, bias],
            [
                shaped(length, width),
                shaped(length, head_width),
                shaped(length, qkv_width),
                shaped(length, kv_local * GROUP * length, dtype=f32),
            ],
            4 * length * width * qkv_width,
        )

    def backward(parts, m, rotated, softmax):
        outs = call(
            functools.partial(backward_kernel, nt, len(parts), kv_local, m),
            [where, *parts, weight_out[m], weight_qkv[m], rotated, softmax, cosine, sine],
            [jax.ShapeDtypeStruct((length, qkv_width), bf16)]
            + [jax.ShapeDtypeStruct((own_rows, width), bf16)] * nt,
            2 * length * width * (qkv_width + head_width),
        )
        return outs[0], outs[1:]

    members = (1, 0)
    x_parts = gather_line(x_rows[0], x_rows[0])
    own_grads = [carried[0], carried[1]]
    first_parts = gather_rotated(carried)
    grad_parts = [first_parts, first_parts]
    normed, attended, rotated, softmax = forward(x_parts)
    normed_peers = peers(normed, True)
    attended_peers = peers(attended, True)
    placed = settled(first_parts)
    shared = send_parts(placed)
    placed, sent_parts = [placed, placed], [shared, shared]
    qkv_lefts, qkv_rights, out_lefts, out_rights = [], [[], []], [], [[], []]
    gain_total = 0.0
    per_tick = []
    for t in range(ticks):
        projected = [None, None]
        partials, received = [None, None], [[], []]
        for m in members:
            projected[m], partials[m] = backward(grad_parts[m], m, rotated, softmax)
            for k in range(1, nt):
                received[m].append(shift(partials[m][k], "tensor", -k))
        projected_peers = [None, None]
        for m in members:
            projected_peers[m] = peers(projected[m], False)
        gain_total = gain_total + call(
            functools.partial(gain_kernel, nt, len(x_parts)),
            [where, *x_parts, *partials[0], *partials[1]],
            [shaped(1, width, dtype=f32)],
            2 * length * width,
        )[0]
        outcome = [None, None]
        for m in members:
            outcome[m] = call(
                functools.partial(norm_kernel, m),
                [where, x_parts[0], own_grads[m], gain[:, 0:1], partials[m][0], *received[m]],
                [jax.ShapeDtypeStruct((own_rows, width), bf16)],
                own_rows * width,
            )[0]
        per_tick.append(jnp.stack(outcome))
        qkv_lefts.extend([slice_for(normed, 0), *normed_peers])
        for m in members:
            qkv_rights[m].extend([projected[m], *projected_peers[m]])
        out_lefts.extend([slice_for(attended, 0), *attended_peers])
        for m in members:
            out_rights[m].extend(placed[m])
            for p in range(nd - 1):
                out_rights[m].extend(g[p] for g in sent_parts[m])
        if t + 1 < ticks:
            later = x_rows[t + 1]
            if t > 0:
                later, _ = lax.optimization_barrier((later, received))
            x_parts = gather_line(later, later)
            normed, attended, rotated, softmax = forward(x_parts)
            normed_peers = peers(normed, True)
            attended_peers = peers(attended, True)
            own_grads, grad_parts = [None, None], [None, None]
            placed, sent_parts = [None, None], [None, None]
            for m in members:
                if m == 1:
                    moves = [(s, s + 1) for s in range(ns - 1)]
                    came = lax.ppermute(outcome[1], "section", moves)
                    own_grads[1] = choose(2, fresh_rows[t], came)
                else:
                    moves = [(s, s - 1) for s in range(1, ns)]
                    came = lax.ppermute(outcome[0], "section", moves)
                    own_grads[0] = choose(1, outcome[1], came)
                grad_parts[m] = gather_rotated(own_grads[m])
                placed[m] = settled(grad_parts[m])
                sent_parts[m] = send_parts(placed[m])

    grad_out = grad_qkv = None
    for m in members:
        grad_out = weight_grad(out_lefts, out_rights[m], False, m, grad_out)
    for m in members:
        grad_qkv = weight_grad(qkv_lefts, qkv_rights[m], True, m, grad_qkv)
    for axis in ("dp", "tensor"):
        gain_total = sum_over(gain_total, axis)
    return (
        jnp.stack(per_tick)[:, :, None, None],
        grad_qkv[:, None],
        grad_out[:, None],
        gain_total,
    )


def solution(mesh):
    in_specs = (
        P(None, None, "section", "dp", "tensor", None),
        P(None, "section", "dp", "tensor", None),
        P(None, "dp", "tensor", None),
        P(None, "section", None, "tensor"),
        P(None, "section", "tensor", None),
        P(None, "section", None),
    )
    out_specs = (
        P(None, None, "section", "dp", "tensor", None),
        P(None, "section", "dp", "tensor"),
        P(None, "section", ("tensor", "dp"), None),
        P(None, "section", None),
    )

    return jax.shard_map(local, mesh=mesh, in_specs=in_specs, out_specs=out_specs, check_vma=False)
```
